256 devices in a mesh: sub: 64 (over x, z, core), tile: 4 (over y).
Axes of the slice: x: 4, y: 4, z: 8, core: 2. Of those that a mesh axis runs over, the one named last changes fastest.
Arguments:
- coupling: bfloat16 [64, 28, 256, 256], P('sub'), may hold values from -0.125 to 0.125
- panel_inv: float32 [64, 8, 256, 256], P('sub')
- a_ib: bfloat16 [64, 2048, 3072], P('sub', None, 'tile'), may hold values from -0.5 to 0.5
- owner: int32 [64, 12, 12], P('sub', None, 'tile'), may hold values from 0 to 63, as said below
- slot: int32 [64, 12, 12], P('sub', None, 'tile'), may hold values from 0 to 15
- base: bfloat16 [64, 64, 256, 256], P('sub', 'tile'), may hold values from -2 to 2
Outputs:
- assembled: bfloat16 [64, 64, 256, 256], P('sub', 'tile')
The draws below stay inside these ranges and needn't reach their ends.
Inputs may be any that keep to these rules, and one draw needn't show every extreme that they name: `owner`: tiles of one device are those of one subdomain s and tile columns t*12/4 to (t+1)*12/4 - 1. At most 1 tiles of one device name one sub index; for each t one sub index, drawn from the seed, is named by exactly 1 tiles of every device of that t.
All inputs are finite; a program needn't handle non-finite values.
Results may differ from the reference program's by a relative error of at most 0.0051.
Values may be sent and summed in bfloat16 or wider, within the bound.
No kernel may reach another device: no remote copies, remote signals or barrier semaphores. Data moves between devices by JAX's collectives and lax.ppermute only.
A program may use at most 128 MiB of HBM per device.

```python
import math
import jax
import jax.numpy as jnp
from jax import lax

NI = 2048
NB = 3072
PANEL = 256
SLOTS = 16
LOWER = 28
NBT = 12
SUBS = 64
OWNED = 64
N_SUB = 64
N_TILE = 4


def draw_panel_inv(key, part):
    random_key = jax.random.fold_in(key, 1)
    shape = (SUBS, NI // PANEL, PANEL, PANEL)
    random_part = jax.random.normal(random_key, shape, jnp.float32)
    identity = jnp.eye(PANEL, dtype=jnp.float32)
    return 0.6 * identity + 0.3 * random_part / math.sqrt(PANEL)


def draw_owner(key, part):
    tile_side = NB // PANEL
    tile_count = tile_side * tile_side // N_TILE
    capacity = (tile_count + N_SUB - 1) // N_SUB
    others = (N_SUB - 1) * capacity
    hot_key, seat_key = jax.random.split(key)
    hottest = jax.random.randint(hot_key, (N_TILE,), 0, N_SUB).astype(jnp.int32)

    def one_device(device_key, hot_owner):
        first_key, second_key = jax.random.split(device_key)
        seat_order = jax.random.permutation(first_key, others)[:tile_count - capacity].astype(jnp.int32)
        chosen = (hot_owner + 1 + seat_order // capacity) % N_SUB
        listed = jnp.concatenate([jnp.full((capacity,), hot_owner, jnp.int32), chosen.astype(jnp.int32)])
        return listed[jax.random.permutation(second_key, tile_count)]
    device_keys = jax.random.split(seat_key, SUBS * N_TILE)
    hot_all = jnp.tile(hottest, SUBS)
    drawn = jax.vmap(one_device)(device_keys, hot_all)
    drawn = drawn.reshape(SUBS, N_TILE, tile_side, tile_count // tile_side)
    return drawn.transpose(0, 2, 1, 3).reshape(SUBS, tile_side, tile_side)


def set_ends(array, rng, least, high):
    extent = array.shape
    index_at = [jax.random.randint(jax.random.fold_in(rng, axis), (), 0, extent[axis]) for axis in range(len(extent))]
    array = array.at[tuple(index_at)].set(least)
    longest = extent.index(max(extent))
    index_at[longest] = (index_at[longest] + 1) % extent[longest]
    return array.at[tuple(index_at)].set(high)


def level_of(stream_key, dims, cuts, low, top_value):
    loudness, own = 1.0, jax.random.fold_in(stream_key, 6)
    for axis_at, parts in cuts:
        steps = jnp.exp(jax.random.uniform(jax.random.fold_in(own, axis_at), (parts,), jnp.float32, low / len(cuts), top_value / len(cuts)))
        loudness = loudness * jnp.repeat(steps, dims[axis_at] // parts).reshape([-1 if axis == axis_at else 1 for axis in range(len(dims))])
    return loudness


def scatter_about(key, shape, scale, most, pieces=(), kind=jnp.bfloat16):
    values = scale * jax.random.normal(key, shape, jnp.float32)
    if pieces:
        values = values * level_of(key, shape, pieces, -0.22, 0.18)
    return jnp.clip(values, -most, most).astype(kind)


def setup_inputs(seed: int = 0) -> dict:
    key_of = jax.random.split(jax.random.key(seed), 7)
    coupling = scatter_about(key_of[0], (SUBS, LOWER, PANEL, PANEL), NI ** -0.5, 0.125, ((0, 64),))
    panel_inv = draw_panel_inv(jax.random.fold_in(key_of[6], 71), 0)
    a_ib = scatter_about(key_of[2], (SUBS, NI, NB), 0.0625, 0.5, ((0, 64), (2, 4)))
    owner = draw_owner(jax.random.fold_in(key_of[6], 71), 0)
    slot = set_ends(jax.random.randint(key_of[4], (SUBS, NBT, NBT), 0, SLOTS), jax.random.fold_in(key_of[4], 1), 0, SLOTS - 1).astype(jnp.int32)
    base = scatter_about(key_of[5], (SUBS, OWNED, PANEL, PANEL), 0.3, 2.0, ((0, 64), (1, 4)))
    return dict(coupling=coupling, panel_inv=panel_inv, a_ib=a_ib, owner=owner, slot=slot, base=base)


def solve(lower_blocks, inverse, right_cols):
    panel_width = inverse.shape[1]
    panels = []
    for row_panel in range(inverse.shape[0]):
        target = right_cols[row_panel * panel_width:(row_panel + 1) * panel_width].astype(jnp.float32)
        if row_panel > 0:
            block_start = row_panel * (row_panel - 1) // 2
            blocks = lower_blocks[block_start:block_start + row_panel]
            joined = jnp.transpose(blocks, (1, 0, 2)).reshape(panel_width, row_panel * panel_width)
            target = target - jnp.dot(joined, jnp.concatenate(panels, axis=0), preferred_element_type=jnp.float32)
        solved_panel = jnp.dot(inverse[row_panel], target, precision=lax.Precision.HIGHEST, preferred_element_type=jnp.float32)
        panels.append(solved_panel.astype(jnp.bfloat16))
    return jnp.concatenate(panels, axis=0)


def reference(coupling, panel_inv, a_ib, owner, slot, base):
    tile_side = NB // PANEL
    col_tiles = tile_side // N_TILE
    column_group = jnp.arange(tile_side, dtype=jnp.int32) // col_tiles

    def assemble_one(accumulated, operands):
        lower_blocks, inverse, right_cols, owner_ids, slot_ids = operands
        solved = solve(lower_blocks, inverse, right_cols)
        gram_matrix = lax.dot_general(solved, solved, (((0,), (0,)), ((), ())), preferred_element_type=jnp.float32)
        contrib = (-gram_matrix).astype(jnp.bfloat16)
        contrib = lax.optimization_barrier(contrib).astype(jnp.float32)
        tiled = contrib.reshape(tile_side, PANEL, tile_side, PANEL).transpose(0, 2, 1, 3)
        places = column_group[None, :] * SLOTS + slot_ids
        accumulated = accumulated.at[owner_ids, places].add(tiled)
        return accumulated, None

    start_total = jnp.zeros((SUBS, OWNED, PANEL, PANEL), jnp.float32)
    accumulated, _ = lax.scan(assemble_one, start_total, (coupling, panel_inv, a_ib, owner, slot))
    return (base.astype(jnp.float32) + accumulated).astype(jnp.bfloat16)
```

```python
import functools

import jax
import jax.numpy as jnp
from jax import lax
from jax.experimental import pallas as pl
from jax.experimental.pallas import tpu as pltpu
from jax.sharding import Mesh
from jax.sharding import PartitionSpec as P

SUB = ("sub_0", "sub_1", "sub_2")
NT = (((1,), (1,)), ((), ()))
CHUNKS = (16, 48, 96, 96)
ROW_BLOCK = 16


def offsets():
    found, total = [], 0
    for rows in CHUNKS:
        found.append(total)
        total += rows
    return found


def solve_kernel(lower_ref, inverse_ref, right_ref, whole_ref, *rest):
    chunk_refs, joined_ref = rest[:-1], rest[-1]
    panels, panel = inverse_ref.shape[0], inverse_ref.shape[1]
    col_tiles = whole_ref.shape[0] // panel
    for k in range(panels):
        target = right_ref[k * panel : (k + 1) * panel, :].astype(jnp.float32).T
        if k > 0:
            first = k * (k - 1) // 2
            for m in range(k):
                joined_ref[:, m * panel : (m + 1) * panel] = lower_ref[first + m]
            target = target - lax.dot_general(
                whole_ref[:, : k * panel],
                joined_ref[:, : k * panel],
                NT,
                preferred_element_type=jnp.float32,
            )
        high = target.astype(jnp.bfloat16)
        low = (target - high.astype(jnp.float32)).astype(jnp.bfloat16)
        inverse = inverse_ref[k]
        inverse_high = inverse.astype(jnp.bfloat16)
        inverse_low = (inverse - inverse_high.astype(jnp.float32)).astype(jnp.bfloat16)
        product = functools.partial(
            lax.dot_general, dimension_numbers=NT, preferred_element_type=jnp.float32
        )
        solved = product(high, inverse_high) + (
            product(low, inverse_high) + product(high, inverse_low)
        )
        whole_ref[:, k * panel : (k + 1) * panel] = solved.astype(jnp.bfloat16)
    for ref, start, rows in zip(chunk_refs, offsets(), CHUNKS):
        for j in range(col_tiles):
            ref[j] = whole_ref[j * panel + start : j * panel + start + rows, :]


def solve(lower_blocks, inverse, right_cols):
    panel = inverse.shape[1]
    inner, cols = right_cols.shape
    col_tiles = cols // panel
    vmem = pl.BlockSpec(memory_space=pltpu.VMEM)
    return pl.pallas_call(
        solve_kernel,
        out_shape=[jax.ShapeDtypeStruct((cols, inner), jnp.bfloat16)]
        + [jax.ShapeDtypeStruct((col_tiles, rows, inner), jnp.bfloat16) for rows in CHUNKS],
        in_specs=[vmem] * 3,
        out_specs=[vmem] * (1 + len(CHUNKS)),
        scratch_shapes=[pltpu.VMEM((panel, inner - panel), jnp.bfloat16)],
        compiler_params=pltpu.CompilerParams(vmem_limit_bytes=40 * 1024 * 1024),
        cost_estimate=pl.CostEstimate(
            flops=12_000_000_000, bytes_accessed=16_000_000, transcendentals=0
        ),
        name="solve",
    )(lower_blocks, inverse, right_cols)


def gram_kernel(place_ref, owner_ref, own_ref, next_ref, far_ref, last_ref, whole_ref, seats_ref, left_ref):
    col_tiles, rows, inner = own_ref.shape
    panel = whole_ref.shape[0] // col_tiles
    groups = (own_ref, next_ref, far_ref, last_ref)
    for step, ref in enumerate(groups):
        for j in range(col_tiles):
            first = (step * col_tiles + j) * rows
            left_ref[first : first + rows, :] = ref[j]
    place = place_ref[0]

    def column(b, carry):
        right = whole_ref[pl.ds(pl.multiple_of(b * panel, panel), panel), :]
        block = lax.dot_general(left_ref[...], right, NT, preferred_element_type=jnp.float32)
        block = (-block).astype(jnp.bfloat16)
        for step in range(len(groups)):
            group = lax.rem(place + step, len(groups))
            for j in range(col_tiles):
                seat = owner_ref[(group * col_tiles + j) * col_tiles + b]
                first = (step * col_tiles + j) * rows
                seats_ref[seat] = block[first : first + rows, :]
        return carry

    lax.fori_loop(0, col_tiles, column, 0)


def gram(place, owners, parts, whole, peers):
    col_tiles, rows, inner = parts[0].shape
    cols = whole.shape[0]
    panel = cols // col_tiles
    vmem = pl.BlockSpec(memory_space=pltpu.VMEM)
    smem = pl.BlockSpec(memory_space=pltpu.SMEM)
    total = len(parts) * col_tiles * rows
    return pl.pallas_call(
        gram_kernel,
        out_shape=jax.ShapeDtypeStruct((peers, rows, panel), jnp.bfloat16),
        in_specs=[smem, smem] + [vmem] * 5,
        out_specs=vmem,
        scratch_shapes=[pltpu.VMEM((total, inner), jnp.bfloat16)],
        compiler_params=pltpu.CompilerParams(vmem_limit_bytes=32 * 1024 * 1024),
        cost_estimate=pl.CostEstimate(
            flops=2 * total * cols * inner,
            bytes_accessed=2 * (total * inner + cols * inner + peers * rows * panel),
            transcendentals=0,
        ),
        name="gram",
    )(place, owners, *parts, whole)


def gather_kernel(label_ref, seats_ref, base_ref, out_ref, total_ref):
    peers = seats_ref.shape[0]
    total_ref[...] = base_ref[...].astype(jnp.float32)

    def one(p, carry):
        label = label_ref[p]

        @pl.when(label >= 0)
        def _():
            total_ref[label] = total_ref[label] + seats_ref[p].astype(jnp.float32)

        return carry

    lax.fori_loop(0, peers, one, 0)
    out_ref[...] = total_ref[...].astype(jnp.bfloat16)


def collect(labels, seats, current, start):
    peers, rows, panel = seats.shape
    slots = current.shape[0]
    shift = start // ROW_BLOCK
    here = lambda i, _: (0, i + shift, 0)
    return pl.pallas_call(
        gather_kernel,
        out_shape=jax.ShapeDtypeStruct(current.shape, current.dtype),
        grid_spec=pltpu.PrefetchScalarGridSpec(
            num_scalar_prefetch=1,
            grid=(rows // ROW_BLOCK,),
            in_specs=[
                pl.BlockSpec((peers, ROW_BLOCK, panel), lambda i, _: (0, i, 0)),
                pl.BlockSpec((slots, ROW_BLOCK, panel), here),
            ],
            out_specs=pl.BlockSpec((slots, ROW_BLOCK, panel), here),
            scratch_shapes=[pltpu.VMEM((slots, ROW_BLOCK, panel), jnp.float32)],
        ),
        input_output_aliases={2: 0},
        compiler_params=pltpu.CompilerParams(vmem_limit_bytes=16 * 1024 * 1024),
        cost_estimate=pl.CostEstimate(
            flops=2 * peers * rows * panel,
            bytes_accessed=2 * (peers + 2 * slots) * rows * panel,
            transcendentals=0,
        ),
        name="collect",
    )(labels, seats, current)


def ring(length, step):
    return [(i, (i + step) % length) for i in range(length)]


def shards(coupling, panel_inv, a_ib, owner, slot, base):
    peers = lax.axis_size(SUB)
    around = lax.axis_size("tile")
    owners = owner[0].reshape(-1)
    slots = slot[0].reshape(-1)
    position = jnp.arange(peers, dtype=jnp.int32)
    selected = position[:, None] == owners[None, :]
    labels = jnp.sum(jnp.where(selected, slots[None, :] + 1, 0), axis=1) - 1
    labels = lax.all_to_all(labels, SUB, split_axis=0, concat_axis=0, tiled=True)
    place = lax.axis_index("tile").astype(jnp.int32).reshape(1)
    whole, *own = solve(coupling[0], panel_inv[0], a_ib[0])
    current = base[0]
    for i, start in enumerate(offsets()):
        part = own[i]
        below = lax.ppermute(part, "tile", ring(around, 1))
        above = lax.ppermute(part, "tile", ring(around, -1))
        if i % 2 == 0:
            far = lax.ppermute(below, "tile", ring(around, 1))
        else:
            far = lax.ppermute(above, "tile", ring(around, -1))
        seats = gram(place, owners, (part, above, far, below), whole, peers)
        seats = lax.all_to_all(seats, SUB, split_axis=0, concat_axis=0, tiled=True)
        current = collect(labels, seats, current, start)
    return current[None]


def solution(mesh):
    torus = Mesh(
        mesh.devices.reshape(4, 8, 2, mesh.shape["tile"]), ("sub_0", "sub_1", "sub_2", "tile")
    )
    placed = (
        P(SUB, None, None, None),
        P(SUB, None, None, None),
        P(SUB, None, "tile"),
        P(SUB, None, "tile"),
        P(SUB, None, "tile"),
        P(SUB, "tile", None, None),
    )
    return jax.shard_map(
        shards, mesh=torus, in_specs=placed, out_specs=P(SUB, "tile", None, None), check_vma=False
    )
```

```python
import functools

import jax
import jax.numpy as jnp
from jax import lax
from jax.experimental import pallas as pl
from jax.experimental.pallas import tpu as pltpu
from jax.sharding import Mesh
from jax.sharding import PartitionSpec as P


SUB = ("sub_0", "sub_1", "sub_2")
NT = (((1,), (1,)), ((), ()))
CHUNKS = (16, 32, 64, 64, 80)


def offsets():
    found, total = [], 0
    for rows in CHUNKS:
        found.append(total)
        total += rows
    return found


def solve_kernel(lower_ref, inverse_ref, right_ref, whole_ref, *rest):
    chunk_refs, joined_ref = rest[:-1], rest[-1]
    panels, panel = inverse_ref.shape[0], inverse_ref.shape[1]
    col_tiles = whole_ref.shape[0] // panel
    for k in range(panels):
        target = right_ref[k * panel : (k + 1) * panel, :].astype(jnp.float32).T
        if k > 0:
            first = k * (k - 1) // 2
            for m in range(k):
                joined_ref[:, m * panel : (m + 1) * panel] = lower_ref[first + m]
            target = target - lax.dot_general(
                whole_ref[:, : k * panel],
                joined_ref[:, : k * panel],
                NT,
                preferred_element_type=jnp.float32,
            )
        high = target.astype(jnp.bfloat16)
        low = (target - high.astype(jnp.float32)).astype(jnp.bfloat16)
        inverse = inverse_ref[k]
        inverse_high = inverse.astype(jnp.bfloat16)
        inverse_low = (inverse - inverse_high.astype(jnp.float32)).astype(jnp.bfloat16)
        product = functools.partial(
            lax.dot_general, dimension_numbers=NT, preferred_element_type=jnp.float32
        )
        solved = product(high, inverse_high) + (
            product(low, inverse_high) + product(high, inverse_low)
        )
        whole_ref[:, k * panel : (k + 1) * panel] = solved.astype(jnp.bfloat16)
    for ref, start, rows in zip(chunk_refs, offsets(), CHUNKS):
        for j in range(col_tiles):
            ref[j] = whole_ref[j * panel + start : j * panel + start + rows, :]


def solve(lower_blocks, inverse, right_cols):
    panel = inverse.shape[1]
    inner, cols = right_cols.shape
    col_tiles = cols // panel
    vmem = pl.BlockSpec(memory_space=pltpu.VMEM)
    return pl.pallas_call(
        solve_kernel,
        out_shape=[jax.ShapeDtypeStruct((cols, inner), jnp.bfloat16)]
        + [jax.ShapeDtypeStruct((col_tiles, rows, inner), jnp.bfloat16) for rows in CHUNKS],
        in_specs=[vmem] * 3,
        out_specs=[vmem] * (1 + len(CHUNKS)),
        scratch_shapes=[pltpu.VMEM((panel, inner - panel), jnp.bfloat16)],
        compiler_params=pltpu.CompilerParams(vmem_limit_bytes=40 * 1024 * 1024),
        cost_estimate=pl.CostEstimate(
            flops=12_000_000_000, bytes_accessed=16_000_000, transcendentals=0
        ),
        name="solve",
    )(lower_blocks, inverse, right_cols)


def gram_kernel(place_ref, seat_ref, own_ref, next_ref, far_ref, last_ref, whole_ref, seats_ref, left_ref):
    col_tiles, rows, _ = own_ref.shape
    panel = whole_ref.shape[0] // col_tiles
    groups = (own_ref, next_ref, far_ref, last_ref)
    for step, ref in enumerate(groups):
        for j in range(col_tiles):
            first = (step * col_tiles + j) * rows
            left_ref[first : first + rows, :] = ref[j]
    place = place_ref[0]

    def column(b, carry):
        right = whole_ref[pl.ds(pl.multiple_of(b * panel, panel), panel), :]
        block = lax.dot_general(left_ref[...], right, NT, preferred_element_type=jnp.float32)
        block = (-block).astype(jnp.bfloat16)
        for step in range(len(groups)):
            group = lax.rem(place + step, len(groups))
            for j in range(col_tiles):
                seat = seat_ref[(group * col_tiles + j) * col_tiles + b]
                first = (step * col_tiles + j) * rows
                seats_ref[seat] = block[first : first + rows, :]
        return carry

    lax.fori_loop(0, col_tiles, column, 0)


def gram(place, seats, parts, whole, peers):
    col_tiles, rows, inner = parts[0].shape
    cols = whole.shape[0]
    panel = cols // col_tiles
    vmem = pl.BlockSpec(memory_space=pltpu.VMEM)
    smem = pl.BlockSpec(memory_space=pltpu.SMEM)
    total = len(parts) * col_tiles * rows
    return pl.pallas_call(
        gram_kernel,
        out_shape=jax.ShapeDtypeStruct((peers, rows, panel), jnp.bfloat16),
        in_specs=[smem, smem] + [vmem] * 5,
        out_specs=vmem,
        scratch_shapes=[pltpu.VMEM((total, inner), jnp.bfloat16)],
        compiler_params=pltpu.CompilerParams(vmem_limit_bytes=32 * 1024 * 1024),
        cost_estimate=pl.CostEstimate(
            flops=2 * total * cols * inner,
            bytes_accessed=2 * (total * inner + cols * inner + peers * rows * panel),
            transcendentals=0,
        ),
        name="gram",
    )(place, seats, *parts, whole)


def row_block(start, rows):
    block = 32
    while start % block or rows % block:
        block //= 2
    return block


def add_by_slot(total_ref, label_ref, tiles_ref, plane, planes, cores):
    def one(p, carry):
        source = ((p // cores) * planes + plane) * cores + p % cores
        label = label_ref[source]

        @pl.when(label >= 0)
        def _():
            tile = tiles_ref[p] if len(tiles_ref.shape) == 3 else tiles_ref[p, 0]
            total_ref[label] = total_ref[label] + tile.astype(jnp.float32)

        return carry

    lax.fori_loop(0, tiles_ref.shape[0], one, 0)


def merge_kernel(above, below, planes, cores, level_ref, up_ref, down_ref, *refs):
    up_raw, down_raw = refs[:above], refs[above : above + below]
    up_own, down_own, up_out, down_out, total_ref = refs[above + below :]
    level = level_ref[0]
    for sign, labels, raw, own, out in (
        (1, up_ref, up_raw, up_own, up_out),
        (-1, down_ref, down_raw, down_own, down_out),
    ):
        total_ref[...] = jnp.zeros_like(total_ref)
        add_by_slot(total_ref, labels, own, level, planes, cores)
        for k, ref in enumerate(raw):
            plane = lax.rem(level - sign * (k + 1) + planes, planes)
            add_by_slot(total_ref, labels, ref, plane, planes, cores)
        out[...] = total_ref[...].astype(jnp.bfloat16)


def merge(level, up_labels, down_labels, up_raw, down_raw, arrived, slots, cores):
    near, planes, rows, panel = arrived.shape
    block = row_block(0, rows)
    tiles = pl.BlockSpec((near, block, panel), lambda i, *_: (0, i, 0))
    dense = pl.BlockSpec((slots, block, panel), lambda i, *_: (0, i, 0))
    own = lambda where: pl.BlockSpec((near, 1, block, panel), lambda i, *_: (0, where, i, 0))
    shape = jax.ShapeDtypeStruct((slots, rows, panel), arrived.dtype)
    count = len(up_raw) + len(down_raw)
    return pl.pallas_call(
        functools.partial(merge_kernel, len(up_raw), len(down_raw), planes, cores),
        out_shape=[shape, shape],
        grid_spec=pltpu.PrefetchScalarGridSpec(
            num_scalar_prefetch=3,
            grid=(rows // block,),
            in_specs=[tiles] * count + [own(1), own(planes - 1)],
            out_specs=[dense, dense],
            scratch_shapes=[pltpu.VMEM((slots, block, panel), jnp.float32)],
        ),
        compiler_params=pltpu.CompilerParams(vmem_limit_bytes=16 * 1024 * 1024),
        cost_estimate=pl.CostEstimate(
            flops=200 * (count + 2) * near * rows * panel,
            bytes_accessed=2 * ((count + 2) * near + 2 * slots) * rows * panel,
            transcendentals=0,
        ),
        name="merge",
    )(level, up_labels, down_labels, *up_raw, *down_raw, arrived, arrived)


def finish_kernel(planes, cores, level_ref, label_ref, own_ref, lower_ref, upper_ref, base_ref, out_ref, total_ref):
    total_ref[...] = base_ref[...].astype(jnp.float32) + (
        lower_ref[...].astype(jnp.float32) + upper_ref[...].astype(jnp.float32)
    )
    add_by_slot(total_ref, label_ref, own_ref, level_ref[0], planes, cores)
    out_ref[...] = total_ref[...].astype(jnp.bfloat16)


def finish(level, labels, arrived, lower, upper, current, start, cores):
    near, planes, rows, panel = arrived.shape
    slots = current.shape[0]
    block = row_block(start, rows)
    shift = start // block
    here = pl.BlockSpec((slots, block, panel), lambda i, *_: (0, i + shift, 0))
    dense = pl.BlockSpec((slots, block, panel), lambda i, *_: (0, i, 0))
    return pl.pallas_call(
        functools.partial(finish_kernel, planes, cores),
        out_shape=jax.ShapeDtypeStruct(current.shape, current.dtype),
        grid_spec=pltpu.PrefetchScalarGridSpec(
            num_scalar_prefetch=2,
            grid=(rows // block,),
            in_specs=[
                pl.BlockSpec((near, 1, block, panel), lambda i, *_: (0, 0, i, 0)),
                dense,
                dense,
                here,
            ],
            out_specs=here,
            scratch_shapes=[pltpu.VMEM((slots, block, panel), jnp.float32)],
        ),
        input_output_aliases={5: 0},
        compiler_params=pltpu.CompilerParams(vmem_limit_bytes=16 * 1024 * 1024),
        cost_estimate=pl.CostEstimate(
            flops=200 * (near + 2 * slots) * rows * panel,
            bytes_accessed=2 * (near + 4 * slots) * rows * panel,
            transcendentals=0,
        ),
        name="finish",
    )(level, labels, arrived, lower, upper, current)


def ring(length, step):
    return [(i, (i + step) % length) for i in range(length)]


def send(array, axis, step):
    return lax.ppermute(array, axis, ring(lax.axis_size(axis), step))


def trade(array, axes):
    return lax.all_to_all(array, axes, split_axis=0, concat_axis=0, tiled=True)


def reaches(planes, i):
    half = planes // 2
    return (half, half - 1) if i % 2 == 0 else (half - 1, half)


def shards(coupling, panel_inv, a_ib, owner, slot, base):
    return assemble(coupling[0], panel_inv[0], a_ib[0], owner[0], slot[0], base[0])[None]


def assemble(lower_blocks, inverse, right_cols, owner, slot, base):
    peers = lax.axis_size(SUB)
    planes, cores = lax.axis_size("sub_1"), lax.axis_size("sub_2")
    near = peers // planes
    slot_count = base.shape[0]
    panel = base.shape[1]
    owners = owner.reshape(-1)
    slots = slot.reshape(-1)
    position = jnp.arange(peers, dtype=jnp.int32)
    selected = position[:, None] == owners[None, :]
    labels = jnp.sum(jnp.where(selected, slots[None, :] + 1, 0), axis=1) - 1
    labels = trade(labels, SUB)
    up_labels = send(labels, "sub_1", -1)
    down_labels = send(labels, "sub_1", 1)
    place = lax.axis_index("tile").astype(jnp.int32).reshape(1)
    level = lax.axis_index("sub_1").astype(jnp.int32)
    distance = (owners // cores - level + planes) % planes
    seat_of = (owners // (planes * cores) * cores + owners % cores) * planes + distance
    level = level.reshape(1)
    whole, *own = solve(lower_blocks, inverse, right_cols)
    current = base
    for i, start in enumerate(offsets()):
        part = own[i]
        below = send(part, "tile", 1)
        above = send(part, "tile", -1)
        far = send(*((below, "tile", 1) if i % 2 == 0 else (above, "tile", -1)))
        seats = gram(place, seat_of, (part, above, far, below), whole, peers)
        seats = seats.reshape(near, planes, part.shape[1], panel)
        arrived = trade(seats, ("sub_0", "sub_2"))
        up_reach, down_reach = reaches(planes, i)
        up_raw = [send(arrived[:, d], "sub_1", d - 1) for d in range(2, up_reach + 1)]
        down_raw = [send(arrived[:, planes - d], "sub_1", 1 - d) for d in range(2, down_reach + 1)]
        up, down = merge(
            level, up_labels, down_labels, up_raw, down_raw, arrived, slot_count, cores
        )
        lower = send(up, "sub_1", 1)
        upper = send(down, "sub_1", -1)
        current = finish(level, labels, arrived, lower, upper, current, start, cores)
    return current


def solution(mesh):
    torus = Mesh(
        mesh.devices.reshape(4, 8, 2, mesh.shape["tile"]), ("sub_0", "sub_1", "sub_2", "tile")
    )
    placed = (
        P(SUB, None, None, None),
        P(SUB, None, None, None),
        P(SUB, None, "tile"),
        P(SUB, None, "tile"),
        P(SUB, None, "tile"),
        P(SUB, "tile", None, None),
    )
    return jax.shard_map(
        shards, mesh=torus, in_specs=placed, out_specs=P(SUB, "tile", None, None), check_vma=False
    )
```

```python
import functools

import jax
import jax.numpy as jnp
from jax import lax
from jax.experimental import pallas as pl
from jax.experimental.pallas import tpu as pltpu
from jax.sharding import Mesh
from jax.sharding import PartitionSpec as P


SUB = ("sub_0", "sub_1", "sub_2")
NT = (((1,), (1,)), ((), ()))
CHUNKS = (16, 48, 96, 96)


def offsets():
    found, total = [], 0
    for rows in CHUNKS:
        found.append(total)
        total += rows
    return found


def solve_kernel(lower_ref, inverse_ref, right_ref, whole_ref, *rest):
    chunk_refs, joined_ref = rest[:-1], rest[-1]
    panels, panel = inverse_ref.shape[0], inverse_ref.shape[1]
    col_tiles = whole_ref.shape[0] // panel
    for k in range(panels):
        target = right_ref[k * panel : (k + 1) * panel, :].astype(jnp.float32).T
        if k > 0:
            first = k * (k - 1) // 2
            for m in range(k):
                joined_ref[:, m * panel : (m + 1) * panel] = lower_ref[first + m]
            target = target - lax.dot_general(
                whole_ref[:, : k * panel],
                joined_ref[:, : k * panel],
                NT,
                preferred_element_type=jnp.float32,
            )
        high = target.astype(jnp.bfloat16)
        low = (target - high.astype(jnp.float32)).astype(jnp.bfloat16)
        inverse = inverse_ref[k]
        inverse_high = inverse.astype(jnp.bfloat16)
        inverse_low = (inverse - inverse_high.astype(jnp.float32)).astype(jnp.bfloat16)
        product = functools.partial(
            lax.dot_general, dimension_numbers=NT, preferred_element_type=jnp.float32
        )
        solved = product(high, inverse_high) + (
            product(low, inverse_high) + product(high, inverse_low)
        )
        whole_ref[:, k * panel : (k + 1) * panel] = solved.astype(jnp.bfloat16)
    for ref, start, rows in zip(chunk_refs, offsets(), CHUNKS):
        for j in range(col_tiles):
            ref[j] = whole_ref[j * panel + start : j * panel + start + rows, :]


def solve(lower_blocks, inverse, right_cols):
    panel = inverse.shape[1]
    inner, cols = right_cols.shape
    col_tiles = cols // panel
    vmem = pl.BlockSpec(memory_space=pltpu.VMEM)
    return pl.pallas_call(
        solve_kernel,
        out_shape=[jax.ShapeDtypeStruct((cols, inner), jnp.bfloat16)]
        + [jax.ShapeDtypeStruct((col_tiles, rows, inner), jnp.bfloat16) for rows in CHUNKS],
        in_specs=[vmem] * 3,
        out_specs=[vmem] * (1 + len(CHUNKS)),
        scratch_shapes=[pltpu.VMEM((panel, inner - panel), jnp.bfloat16)],
        compiler_params=pltpu.CompilerParams(vmem_limit_bytes=40 * 1024 * 1024),
        cost_estimate=pl.CostEstimate(
            flops=12_000_000_000, bytes_accessed=16_000_000, transcendentals=0
        ),
        name="solve",
    )(lower_blocks, inverse, right_cols)


def gram_kernel(place_ref, owner_ref, own_ref, next_ref, far_ref, last_ref, whole_ref, seats_ref, left_ref):
    col_tiles, rows, _ = own_ref.shape
    panel = whole_ref.shape[0] // col_tiles
    groups = (own_ref, next_ref, far_ref, last_ref)
    for step, ref in enumerate(groups):
        for j in range(col_tiles):
            first = (step * col_tiles + j) * rows
            left_ref[first : first + rows, :] = ref[j]
    place = place_ref[0]

    def column(b, carry):
        right = whole_ref[pl.ds(pl.multiple_of(b * panel, panel), panel), :]
        block = lax.dot_general(left_ref[...], right, NT, preferred_element_type=jnp.float32)
        block = (-block).astype(jnp.bfloat16)
        for step in range(len(groups)):
            group = lax.rem(place + step, len(groups))
            for j in range(col_tiles):
                seat = owner_ref[(group * col_tiles + j) * col_tiles + b]
                first = (step * col_tiles + j) * rows
                seats_ref[seat] = block[first : first + rows, :]
        return carry

    lax.fori_loop(0, col_tiles, column, 0)


def gram(place, owners, parts, whole, peers):
    col_tiles, rows, inner = parts[0].shape
    cols = whole.shape[0]
    panel = cols // col_tiles
    vmem = pl.BlockSpec(memory_space=pltpu.VMEM)
    smem = pl.BlockSpec(memory_space=pltpu.SMEM)
    total = len(parts) * col_tiles * rows
    return pl.pallas_call(
        gram_kernel,
        out_shape=jax.ShapeDtypeStruct((peers, rows, panel), jnp.bfloat16),
        in_specs=[smem, smem] + [vmem] * 5,
        out_specs=vmem,
        scratch_shapes=[pltpu.VMEM((total, inner), jnp.bfloat16)],
        compiler_params=pltpu.CompilerParams(vmem_limit_bytes=32 * 1024 * 1024),
        cost_estimate=pl.CostEstimate(
            flops=2 * total * cols * inner,
            bytes_accessed=2 * (total * inner + cols * inner + peers * rows * panel),
            transcendentals=0,
        ),
        name="gram",
    )(place, owners, *parts, whole)


def row_block(start, rows):
    block = 32
    while start % block or rows % block:
        block //= 2
    return block


def collect_kernel(label_ref, seats_ref, base_ref, *refs):
    out_ref, total_ref = refs[-2:]
    total_ref[...] = base_ref[...].astype(jnp.float32)

    def one(p, carry):
        label = label_ref[p]

        @pl.when(label >= 0)
        def _():
            total_ref[label] = total_ref[label] + seats_ref[p].astype(jnp.float32)

        return carry

    lax.fori_loop(0, seats_ref.shape[0], one, 0, unroll=4)
    out_ref[...] = total_ref[...].astype(jnp.bfloat16)


def collect(labels, seats, base, current, start):
    peers, rows, panel = seats.shape
    slots = base.shape[0]
    block = row_block(start, rows)
    shift = start // block
    here = pl.BlockSpec((slots, block, panel), lambda i, _: (0, i + shift, 0))
    before = [] if current is None else [current]
    return pl.pallas_call(
        collect_kernel,
        out_shape=jax.ShapeDtypeStruct(base.shape, base.dtype),
        grid_spec=pltpu.PrefetchScalarGridSpec(
            num_scalar_prefetch=1,
            grid=(rows // block,),
            in_specs=[pl.BlockSpec((peers, block, panel), lambda i, _: (0, i, 0)), here]
            + [pl.BlockSpec(memory_space=pl.ANY)] * len(before),
            out_specs=here,
            scratch_shapes=[pltpu.VMEM((slots, block, panel), jnp.float32)],
        ),
        input_output_aliases={3: 0} if before else {},
        compiler_params=pltpu.CompilerParams(vmem_limit_bytes=16 * 1024 * 1024),
        cost_estimate=pl.CostEstimate(
            flops=2 * peers * rows * panel,
            bytes_accessed=2 * (peers + 2 * slots) * rows * panel,
            transcendentals=0,
        ),
        name="collect",
    )(labels, seats, base, *before)


def ring(length, step):
    return [(i, (i + step) % length) for i in range(length)]


def send(array, axis, step):
    return lax.ppermute(array, axis, ring(lax.axis_size(axis), step))


def trade(array, axes):
    return lax.all_to_all(array, axes, split_axis=0, concat_axis=0, tiled=True)


def shards(coupling, panel_inv, a_ib, owner, slot, base):
    return assemble(coupling[0], panel_inv[0], a_ib[0], owner[0], slot[0], base[0])[None]


def assemble(lower_blocks, inverse, right_cols, owner, slot, base):
    peers = lax.axis_size(SUB)
    owners = owner.reshape(-1)
    slots = slot.reshape(-1)
    position = jnp.arange(peers, dtype=jnp.int32)
    selected = position[:, None] == owners[None, :]
    labels = jnp.sum(jnp.where(selected, slots[None, :] + 1, 0), axis=1) - 1
    labels = trade(labels, SUB)
    place = lax.axis_index("tile").astype(jnp.int32).reshape(1)
    whole, *own = solve(lower_blocks, inverse, right_cols)
    current = None
    for i, start in enumerate(offsets()):
        part = own[i]
        below = send(part, "tile", 1)
        above = send(part, "tile", -1)
        far = send(*((below, "tile", 1) if i % 2 == 0 else (above, "tile", -1)))
        seats = gram(place, owners, (part, above, far, below), whole, peers)
        seats = trade(seats, SUB)
        current = collect(labels, seats, base, current, start)
    return current


def solution(mesh):
    torus = Mesh(
        mesh.devices.reshape(4, 8, 2, mesh.shape["tile"]), ("sub_0", "sub_1", "sub_2", "tile")
    )
    placed = (
        P(SUB, None, None, None),
        P(SUB, None, None, None),
        P(SUB, None, "tile"),
        P(SUB, None, "tile"),
        P(SUB, None, "tile"),
        P(SUB, "tile", None, None),
    )
    return jax.shard_map(
        shards, mesh=torus, in_specs=placed, out_specs=P(SUB, "tile", None, None), check_vma=False
    )
```

```python
import functools

import jax
import jax.numpy as jnp
from jax import lax
from jax.experimental import pallas as pl
from jax.experimental.pallas import tpu as pltpu
from jax.sharding import Mesh
from jax.sharding import PartitionSpec as P


SUB = ("sub_0", "sub_1", "sub_2")
NT = (((1,), (1,)), ((), ()))
CHUNKS = (16, 48, 64, 64, 64)


def offsets():
    found, total = [], 0
    for rows in CHUNKS:
        found.append(total)
        total += rows
    return found


def solve_kernel(lower_ref, inverse_ref, right_ref, whole_ref, *rest):
    chunk_refs, joined_ref = rest[:-1], rest[-1]
    panels, panel = inverse_ref.shape[0], inverse_ref.shape[1]
    col_tiles = whole_ref.shape[0] // panel
    for k in range(panels):
        target = right_ref[k * panel : (k + 1) * panel, :].astype(jnp.float32).T
        if k > 0:
            first = k * (k - 1) // 2
            for m in range(k):
                joined_ref[:, m * panel : (m + 1) * panel] = lower_ref[first + m]
            target = target - lax.dot_general(
                whole_ref[:, : k * panel],
                joined_ref[:, : k * panel],
                NT,
                preferred_element_type=jnp.float32,
            )
        high = target.astype(jnp.bfloat16)
        low = (target - high.astype(jnp.float32)).astype(jnp.bfloat16)
        inverse = inverse_ref[k]
        inverse_high = inverse.astype(jnp.bfloat16)
        inverse_low = (inverse - inverse_high.astype(jnp.float32)).astype(jnp.bfloat16)
        product = functools.partial(
            lax.dot_general, dimension_numbers=NT, preferred_element_type=jnp.float32
        )
        solved = product(high, inverse_high) + (
            product(low, inverse_high) + product(high, inverse_low)
        )
        whole_ref[:, k * panel : (k + 1) * panel] = solved.astype(jnp.bfloat16)
    for ref, start, rows in zip(chunk_refs, offsets(), CHUNKS):
        for j in range(col_tiles):
            ref[j] = whole_ref[j * panel + start : j * panel + start + rows, :]


def solve(lower_blocks, inverse, right_cols):
    panel = inverse.shape[1]
    inner, cols = right_cols.shape
    col_tiles = cols // panel
    vmem = pl.BlockSpec(memory_space=pltpu.VMEM)
    return pl.pallas_call(
        solve_kernel,
        out_shape=[jax.ShapeDtypeStruct((cols, inner), jnp.bfloat16)]
        + [jax.ShapeDtypeStruct((col_tiles, rows, inner), jnp.bfloat16) for rows in CHUNKS],
        in_specs=[vmem] * 3,
        out_specs=[vmem] * (1 + len(CHUNKS)),
        scratch_shapes=[pltpu.VMEM((panel, inner - panel), jnp.bfloat16)],
        compiler_params=pltpu.CompilerParams(vmem_limit_bytes=40 * 1024 * 1024),
        cost_estimate=pl.CostEstimate(
            flops=12_000_000_000, bytes_accessed=16_000_000, transcendentals=0
        ),
        name="solve",
    )(lower_blocks, inverse, right_cols)


def gram_kernel(place_ref, seat_ref, own_ref, next_ref, far_ref, last_ref, whole_ref, seats_ref, left_ref):
    col_tiles, rows, _ = own_ref.shape
    panel = whole_ref.shape[0] // col_tiles
    groups = (own_ref, next_ref, far_ref, last_ref)
    for step, ref in enumerate(groups):
        for j in range(col_tiles):
            first = (step * col_tiles + j) * rows
            left_ref[first : first + rows, :] = ref[j]
    place = place_ref[0]

    def column(b, carry):
        right = whole_ref[pl.ds(pl.multiple_of(b * panel, panel), panel), :]
        block = lax.dot_general(left_ref[...], right, NT, preferred_element_type=jnp.float32)
        block = (-block).astype(jnp.bfloat16)
        for step in range(len(groups)):
            group = lax.rem(place + step, len(groups))
            for j in range(col_tiles):
                seat = seat_ref[(group * col_tiles + j) * col_tiles + b]
                first = (step * col_tiles + j) * rows
                seats_ref[seat] = block[first : first + rows, :]
        return carry

    lax.fori_loop(0, col_tiles, column, 0)


def gram(place, seats, parts, whole, peers):
    col_tiles, rows, inner = parts[0].shape
    cols = whole.shape[0]
    panel = cols // col_tiles
    vmem = pl.BlockSpec(memory_space=pltpu.VMEM)
    smem = pl.BlockSpec(memory_space=pltpu.SMEM)
    total = len(parts) * col_tiles * rows
    return pl.pallas_call(
        gram_kernel,
        out_shape=jax.ShapeDtypeStruct((peers, rows, panel), jnp.bfloat16),
        in_specs=[smem, smem] + [vmem] * 5,
        out_specs=vmem,
        scratch_shapes=[pltpu.VMEM((total, inner), jnp.bfloat16)],
        compiler_params=pltpu.CompilerParams(vmem_limit_bytes=32 * 1024 * 1024),
        cost_estimate=pl.CostEstimate(
            flops=2 * total * cols * inner,
            bytes_accessed=2 * (total * inner + cols * inner + peers * rows * panel),
            transcendentals=0,
        ),
        name="gram",
    )(place, seats, *parts, whole)


def row_block(start, rows):
    block = 32
    while start % block or rows % block:
        block //= 2
    return block


def add_by_slot(total_ref, label_ref, tiles_ref, plane):
    near = tiles_ref.shape[0]
    first = plane * near

    def one(p, carry):
        label = label_ref[first + p]

        @pl.when(label >= 0)
        def _():
            tile = tiles_ref[p] if len(tiles_ref.shape) == 3 else tiles_ref[p, 0]
            total_ref[label] = total_ref[label] + tile.astype(jnp.float32)

        return carry

    lax.fori_loop(0, near, one, 0, unroll=2)


def merge_kernel(above, below, planes, level_ref, up_ref, down_ref, *refs):
    up_raw, down_raw = refs[:above], refs[above : above + below]
    up_own, down_own, up_out, down_out, total_ref = refs[above + below :]
    level = level_ref[0]
    for sign, labels, raw, own, out in (
        (1, up_ref, up_raw, up_own, up_out),
        (-1, down_ref, down_raw, down_own, down_out),
    ):
        total_ref[...] = jnp.zeros_like(total_ref)
        add_by_slot(total_ref, labels, own, level)
        for k, ref in enumerate(raw):
            plane = lax.rem(level - sign * (k + 1) + planes, planes)
            add_by_slot(total_ref, labels, ref, plane)
        out[...] = total_ref[...].astype(jnp.bfloat16)


def merge(level, up_labels, down_labels, up_raw, down_raw, arrived, slots):
    near, planes, rows, panel = arrived.shape
    block = row_block(0, rows)
    tiles = pl.BlockSpec((near, block, panel), lambda i, *_: (0, i, 0))
    dense = pl.BlockSpec((slots, block, panel), lambda i, *_: (0, i, 0))
    own = lambda where: pl.BlockSpec((near, 1, block, panel), lambda i, *_: (0, where, i, 0))
    shape = jax.ShapeDtypeStruct((slots, rows, panel), arrived.dtype)
    count = len(up_raw) + len(down_raw)
    return pl.pallas_call(
        functools.partial(merge_kernel, len(up_raw), len(down_raw), planes),
        out_shape=[shape, shape],
        grid_spec=pltpu.PrefetchScalarGridSpec(
            num_scalar_prefetch=3,
            grid=(rows // block,),
            in_specs=[tiles] * count + [own(1), own(planes - 1)],
            out_specs=[dense, dense],
            scratch_shapes=[pltpu.VMEM((slots, block, panel), jnp.float32)],
        ),
        compiler_params=pltpu.CompilerParams(vmem_limit_bytes=16 * 1024 * 1024),
        cost_estimate=pl.CostEstimate(
            flops=200 * (count + 2) * near * rows * panel,
            bytes_accessed=2 * ((count + 2) * near + 2 * slots) * rows * panel,
            transcendentals=0,
        ),
        name="merge",
    )(level, up_labels, down_labels, *up_raw, *down_raw, arrived, arrived)


def finish_kernel(level_ref, label_ref, own_ref, lower_ref, upper_ref, base_ref, *refs):
    out_ref, total_ref = refs[-2:]
    total_ref[...] = base_ref[...].astype(jnp.float32) + (
        lower_ref[...].astype(jnp.float32) + upper_ref[...].astype(jnp.float32)
    )
    add_by_slot(total_ref, label_ref, own_ref, level_ref[0])
    out_ref[...] = total_ref[...].astype(jnp.bfloat16)


def finish(level, labels, arrived, lower, upper, base, current, start):
    near, _, rows, panel = arrived.shape
    slots = base.shape[0]
    block = row_block(start, rows)
    shift = start // block
    here = pl.BlockSpec((slots, block, panel), lambda i, *_: (0, i + shift, 0))
    dense = pl.BlockSpec((slots, block, panel), lambda i, *_: (0, i, 0))
    before = [] if current is None else [current]
    return pl.pallas_call(
        finish_kernel,
        out_shape=jax.ShapeDtypeStruct(base.shape, base.dtype),
        grid_spec=pltpu.PrefetchScalarGridSpec(
            num_scalar_prefetch=2,
            grid=(rows // block,),
            in_specs=[
                pl.BlockSpec((near, 1, block, panel), lambda i, *_: (0, 0, i, 0)),
                dense,
                dense,
                here,
            ]
            + [pl.BlockSpec(memory_space=pl.ANY)] * len(before),
            out_specs=here,
            scratch_shapes=[pltpu.VMEM((slots, block, panel), jnp.float32)],
        ),
        input_output_aliases={6: 0} if before else {},
        compiler_params=pltpu.CompilerParams(vmem_limit_bytes=16 * 1024 * 1024),
        cost_estimate=pl.CostEstimate(
            flops=200 * (near + 2 * slots) * rows * panel,
            bytes_accessed=2 * (near + 4 * slots) * rows * panel,
            transcendentals=0,
        ),
        name="finish",
    )(level, labels, arrived, lower, upper, base, *before)


def ring(length, step):
    return [(i, (i + step) % length) for i in range(length)]


def send(array, axis, step):
    return lax.ppermute(array, axis, ring(lax.axis_size(axis), step))


def trade(array, axes):
    return lax.all_to_all(array, axes, split_axis=0, concat_axis=0, tiled=True)


def reaches(planes, i):
    half = planes // 2
    return (half, half - 1) if i % 2 == 0 else (half - 1, half)


def shards(coupling, panel_inv, a_ib, owner, slot, base):
    return assemble(coupling[0], panel_inv[0], a_ib[0], owner[0], slot[0], base[0])[None]


def assemble(lower_blocks, inverse, right_cols, owner, slot, base):
    peers = lax.axis_size(SUB)
    planes, cores = lax.axis_size("sub_1"), lax.axis_size("sub_2")
    near = peers // planes
    slot_count = base.shape[0]
    panel = base.shape[1]
    owners = owner.reshape(-1)
    slots = slot.reshape(-1)
    position = jnp.arange(peers, dtype=jnp.int32)
    selected = position[:, None] == owners[None, :]
    labels = jnp.sum(jnp.where(selected, slots[None, :] + 1, 0), axis=1) - 1
    labels = trade(labels, SUB)
    labels = labels.reshape(-1, planes, cores).transpose(1, 0, 2).reshape(peers)
    up_labels = send(labels, "sub_1", -1)
    down_labels = send(labels, "sub_1", 1)
    place = lax.axis_index("tile").astype(jnp.int32).reshape(1)
    level = lax.axis_index("sub_1").astype(jnp.int32)
    distance = (owners // cores - level + planes) % planes
    seat_of = (owners // (planes * cores) * cores + owners % cores) * planes + distance
    level = level.reshape(1)
    whole, *own = solve(lower_blocks, inverse, right_cols)
    current = None
    for i, start in enumerate(offsets()):
        part = own[i]
        below = send(part, "tile", 1)
        above = send(part, "tile", -1)
        far = send(part, "tile", 2)
        seats = gram(place, seat_of, (part, above, far, below), whole, peers)
        seats = seats.reshape(near, planes, part.shape[1], panel)
        arrived = trade(seats, ("sub_0", "sub_2"))
        up_reach, down_reach = reaches(planes, i)
        up_raw = [send(arrived[:, d], "sub_1", d - 1) for d in range(2, up_reach + 1)]
        down_raw = [send(arrived[:, planes - d], "sub_1", 1 - d) for d in range(2, down_reach + 1)]
        up, down = merge(
            level, up_labels, down_labels, up_raw, down_raw, arrived, slot_count
        )
        lower = send(up, "sub_1", 1)
        upper = send(down, "sub_1", -1)
        current = finish(level, labels, arrived, lower, upper, base, current, start)
    return current


def solution(mesh):
    torus = Mesh(
        mesh.devices.reshape(4, 8, 2, mesh.shape["tile"]), ("sub_0", "sub_1", "sub_2", "tile")
    )
    placed = (
        P(SUB, None, None, None),
        P(SUB, None, None, None),
        P(SUB, None, "tile"),
        P(SUB, None, "tile"),
        P(SUB, None, "tile"),
        P(SUB, "tile", None, None),
    )
    return jax.shard_map(
        shards, mesh=torus, in_specs=placed, out_specs=P(SUB, "tile", None, None), check_vma=False
    )
```

```python
import functools

import jax
import jax.numpy as jnp
from jax import lax
from jax.experimental import pallas as pl
from jax.experimental.pallas import tpu as pltpu
from jax.sharding import Mesh
from jax.sharding import PartitionSpec as P


SUB = ("sub_0", "sub_1", "sub_2")
NT = (((1,), (1,)), ((), ()))
CHUNKS = (32, 64, 96, 64)


def offsets():
    found, total = [], 0
    for rows in CHUNKS:
        found.append(total)
        total += rows
    return found


def solve_kernel(lower_ref, inverse_ref, right_ref, whole_ref, *rest):
    chunk_refs, joined_ref = rest[:-1], rest[-1]
    panels, panel = inverse_ref.shape[0], inverse_ref.shape[1]
    col_tiles = whole_ref.shape[0] // panel
    for k in range(panels):
        target = right_ref[k * panel : (k + 1) * panel, :].astype(jnp.float32).T
        if k > 0:
            first = k * (k - 1) // 2
            for m in range(k):
                joined_ref[:, m * panel : (m + 1) * panel] = lower_ref[first + m]
            target = target - lax.dot_general(
                whole_ref[:, : k * panel],
                joined_ref[:, : k * panel],
                NT,
                preferred_element_type=jnp.float32,
            )
        high = target.astype(jnp.bfloat16)
        low = (target - high.astype(jnp.float32)).astype(jnp.bfloat16)
        inverse = inverse_ref[k]
        inverse_high = inverse.astype(jnp.bfloat16)
        inverse_low = (inverse - inverse_high.astype(jnp.float32)).astype(jnp.bfloat16)
        product = functools.partial(
            lax.dot_general, dimension_numbers=NT, preferred_element_type=jnp.float32
        )
        solved = product(high, inverse_high) + (
            product(low, inverse_high) + product(high, inverse_low)
        )
        whole_ref[:, k * panel : (k + 1) * panel] = solved.astype(jnp.bfloat16)
    for ref, start, rows in zip(chunk_refs, offsets(), CHUNKS):
        for j in range(col_tiles):
            ref[j] = whole_ref[j * panel + start : j * panel + start + rows, :]


def solve(lower_blocks, inverse, right_cols):
    panel = inverse.shape[1]
    inner, cols = right_cols.shape
    col_tiles = cols // panel
    vmem = pl.BlockSpec(memory_space=pltpu.VMEM)
    return pl.pallas_call(
        solve_kernel,
        out_shape=[jax.ShapeDtypeStruct((cols, inner), jnp.bfloat16)]
        + [jax.ShapeDtypeStruct((col_tiles, rows, inner), jnp.bfloat16) for rows in CHUNKS],
        in_specs=[vmem] * 3,
        out_specs=[vmem] * (1 + len(CHUNKS)),
        scratch_shapes=[pltpu.VMEM((panel, inner - panel), jnp.bfloat16)],
        compiler_params=pltpu.CompilerParams(vmem_limit_bytes=40 * 1024 * 1024),
        cost_estimate=pl.CostEstimate(
            flops=12_000_000_000, bytes_accessed=16_000_000, transcendentals=0
        ),
        name="solve",
    )(lower_blocks, inverse, right_cols)


def gram_kernel(place_ref, owner_ref, own_ref, next_ref, far_ref, last_ref, whole_ref, seats_ref, left_ref):
    col_tiles, rows, _ = own_ref.shape
    panel = whole_ref.shape[0] // col_tiles
    groups = (own_ref, next_ref, far_ref, last_ref)
    for step, ref in enumerate(groups):
        for j in range(col_tiles):
            first = (step * col_tiles + j) * rows
            left_ref[first : first + rows, :] = ref[j]
    place = place_ref[0]

    def column(b, carry):
        right = whole_ref[pl.ds(pl.multiple_of(b * panel, panel), panel), :]
        block = lax.dot_general(left_ref[...], right, NT, preferred_element_type=jnp.float32)
        block = (-block).astype(jnp.bfloat16)
        for step in range(len(groups)):
            group = lax.rem(place + step, len(groups))
            for j in range(col_tiles):
                seat = owner_ref[(group * col_tiles + j) * col_tiles + b]
                first = (step * col_tiles + j) * rows
                seats_ref[seat] = block[first : first + rows, :]
        return carry

    lax.fori_loop(0, col_tiles, column, 0)


def gram(place, owners, parts, whole, peers):
    col_tiles, rows, inner = parts[0].shape
    cols = whole.shape[0]
    panel = cols // col_tiles
    vmem = pl.BlockSpec(memory_space=pltpu.VMEM)
    smem = pl.BlockSpec(memory_space=pltpu.SMEM)
    total = len(parts) * col_tiles * rows
    return pl.pallas_call(
        gram_kernel,
        out_shape=jax.ShapeDtypeStruct((peers, rows, panel), jnp.bfloat16),
        in_specs=[smem, smem] + [vmem] * 5,
        out_specs=vmem,
        scratch_shapes=[pltpu.VMEM((total, inner), jnp.bfloat16)],
        compiler_params=pltpu.CompilerParams(vmem_limit_bytes=32 * 1024 * 1024),
        cost_estimate=pl.CostEstimate(
            flops=2 * total * cols * inner,
            bytes_accessed=2 * (total * inner + cols * inner + peers * rows * panel),
            transcendentals=0,
        ),
        name="gram",
    )(place, owners, *parts, whole)


def row_block(start, rows):
    block = 32
    while start % block or rows % block:
        block //= 2
    return block


def collect_kernel(core_ref, label_ref, own_ref, other_ref, base_ref, *refs):
    out_ref, total_ref = refs[-2:]
    total_ref[...] = base_ref[...].astype(jnp.float32)
    chips = own_ref.shape[0]
    cores = label_ref.shape[0] // chips
    core = core_ref[0]

    def one(p, carry):
        own = label_ref[p * cores + core]
        other = label_ref[p * cores + cores - 1 - core]

        @pl.when(own >= 0)
        def _():
            total_ref[own] = total_ref[own] + own_ref[p, 0].astype(jnp.float32)

        @pl.when(other >= 0)
        def _():
            total_ref[other] = total_ref[other] + other_ref[p].astype(jnp.float32)

        return carry

    lax.fori_loop(0, chips, one, 0, unroll=2)
    out_ref[...] = total_ref[...].astype(jnp.bfloat16)


def collect(core, labels, arrived, other, base, current, start):
    chips, _, rows, panel = arrived.shape
    slots = base.shape[0]
    block = row_block(start, rows)
    shift = start // block
    here = pl.BlockSpec((slots, block, panel), lambda i, *_: (0, i + shift, 0))
    before = [] if current is None else [current]
    return pl.pallas_call(
        collect_kernel,
        out_shape=jax.ShapeDtypeStruct(base.shape, base.dtype),
        grid_spec=pltpu.PrefetchScalarGridSpec(
            num_scalar_prefetch=2,
            grid=(rows // block,),
            in_specs=[
                pl.BlockSpec((chips, 1, block, panel), lambda i, *_: (0, 0, i, 0)),
                pl.BlockSpec((chips, block, panel), lambda i, *_: (0, i, 0)),
                here,
            ]
            + [pl.BlockSpec(memory_space=pl.ANY)] * len(before),
            out_specs=here,
            scratch_shapes=[pltpu.VMEM((slots, block, panel), jnp.float32)],
        ),
        input_output_aliases={5: 0} if before else {},
        compiler_params=pltpu.CompilerParams(vmem_limit_bytes=16 * 1024 * 1024),
        cost_estimate=pl.CostEstimate(
            flops=4 * chips * rows * panel,
            bytes_accessed=4 * (chips + slots) * rows * panel,
            transcendentals=0,
        ),
        name="collect",
    )(core, labels, arrived, other, base, *before)


def ring(length, step):
    return [(i, (i + step) % length) for i in range(length)]


def send(array, axis, step):
    return lax.ppermute(array, axis, ring(lax.axis_size(axis), step))


def trade(array, axes):
    return lax.all_to_all(array, axes, split_axis=0, concat_axis=0, tiled=True)


def shards(coupling, panel_inv, a_ib, owner, slot, base):
    return assemble(coupling[0], panel_inv[0], a_ib[0], owner[0], slot[0], base[0])[None]


def assemble(lower_blocks, inverse, right_cols, owner, slot, base):
    peers = lax.axis_size(SUB)
    owners = owner.reshape(-1)
    slots = slot.reshape(-1)
    position = jnp.arange(peers, dtype=jnp.int32)
    selected = position[:, None] == owners[None, :]
    labels = jnp.sum(jnp.where(selected, slots[None, :] + 1, 0), axis=1) - 1
    labels = trade(labels, SUB)
    place = lax.axis_index("tile").astype(jnp.int32).reshape(1)
    cores = lax.axis_size("sub_2")
    core = lax.axis_index("sub_2").astype(jnp.int32)
    seat_of = owners // cores * cores + (owners - core + cores) % cores
    core = core.reshape(1)
    whole, *own = solve(lower_blocks, inverse, right_cols)
    current = None
    for i, start in enumerate(offsets()):
        part = own[i]
        below = send(part, "tile", 1)
        above = send(part, "tile", -1)
        far = send(part, "tile", 2)
        seats = gram(place, seat_of, (part, above, far, below), whole, peers)
        seats = seats.reshape(peers // cores, cores, part.shape[1], base.shape[1])
        arrived = trade(seats, ("sub_0", "sub_1"))
        other = send(arrived[:, 1], "sub_2", 1)
        current = collect(core, labels, arrived, other, base, current, start)
    return current


def solution(mesh):
    torus = Mesh(
        mesh.devices.reshape(4, 8, 2, mesh.shape["tile"]), ("sub_0", "sub_1", "sub_2", "tile")
    )
    placed = (
        P(SUB, None, None, None),
        P(SUB, None, None, None),
        P(SUB, None, "tile"),
        P(SUB, None, "tile"),
        P(SUB, None, "tile"),
        P(SUB, "tile", None, None),
    )
    return jax.shard_map(
        shards, mesh=torus, in_specs=placed, out_specs=P(SUB, "tile", None, None), check_vma=False
    )
```
